32 devices in a mesh: dp: 2 (over y), expert: 8 (over z, x), etp: 2 (over core).
Axes of the slice: x: 2, y: 2, z: 4, core: 2. Of those that a mesh axis runs over, the one named last changes fastest.
Arguments:
- tokens: bfloat16 [1024, 4096], P(('dp', 'expert'), 'etp'), may hold values from -6 to 6
- expert_ids: int32 [1024, 8], P(('dp', 'expert')), may hold values from 0 to 15, all different within a row; in each aligned block of 64 rows (0 to 63, 64 to 127, ...) at most 48 rows name the same one
- combine: float32 [1024, 8], P(('dp', 'expert')), may hold values from 0.05 to 1
- gate_weight: bfloat16 [16, 4096, 1536], P('expert', 'dp', 'etp'), may hold values from -0.09375 to 0.09375
- up_weight: bfloat16 [16, 4096, 1536], P('expert', 'dp', 'etp'), may hold values from -0.09375 to 0.09375
- down_weight: bfloat16 [16, 1536, 4096], P('expert', 'etp', 'dp'), may hold values from -0.15625 to 0.15625
Outputs:
- mixed: bfloat16 [1024, 4096], P(('dp', 'expert'), 'etp')
The draws below stay inside these ranges and needn't reach their ends.
Inputs may be any that keep to these rules, and one draw needn't show every extreme that they name: `expert_ids`: each row names 8 different experts. In the rows of one device (aligned blocks of 64 rows) no expert is named by more than 48 rows, a bound that some block reaches.
All inputs are finite; a program needn't handle non-finite values.
Results may differ from the reference program's by a relative error of at most 0.008.
Values may be sent and summed in bfloat16 or wider, within the bound.
A program may use at most 192 MiB of HBM per device.

```python
import math
import jax
import jax.numpy as jnp
import numpy as np
from jax import lax

D = 4096
FF = 1536
TOP = 8
TOK_DEV = 64
EXPERTS = 16
TOKENS = 1024
CAP = 48
N_DP = 2
N_EXPERT = 8
N_ETP = 2


def block_scale(rng, shape, pieces, smallest, high):
    level = 1.0
    for axis_at, blocks in pieces:
        steps = jax.random.uniform(jax.random.fold_in(jax.random.fold_in(rng, 6), axis_at), (blocks,), jnp.float32, smallest / len(pieces), high / len(pieces))
        level = level * jnp.repeat(jnp.exp(steps), shape[axis_at] // blocks).reshape((-1,) + (1,) * (len(shape) - 1 - axis_at))
    return level


def routed_block(own_key, own, number, rows, count, top, limit, lean):
    order = jax.random.permutation(own_key, count)
    heavy_load, common = shares(count, rows * top, limit, lean, True), shares(count, rows * top, limit, lean, False)
    places = jnp.arange(count)

    def named(tallies, turn):
        used = int((tallies > 0).sum())
        fixed = max(1, used // 4)
        shifted = fixed + (places - fixed + turn * (used - fixed)) % max(1, count - fixed)
        return jnp.zeros((count,), jnp.int32).at[order[jnp.where(places < fixed, places, shifted)]].set(jnp.asarray(tallies, jnp.int32))

    tallies = jnp.where(number % 4 == 0, named(heavy_load, number // 4), named(common, number - number // 4 - 1))
    mixed = jax.random.permutation(jax.random.fold_in(own, 3), count)
    source_of, sink = mixed[0:count // 2 * 2:2], mixed[1:count // 2 * 2:2]
    slack = jnp.minimum(tallies[source_of] - 1, limit - tallies[sink]) // 2
    slack = jnp.where((source_of == order[0]) | (sink == order[0]) | (tallies[sink] == 0), 0, jnp.maximum(slack, 0))
    shifted = jax.random.randint(jax.random.fold_in(own, 4), (count // 2,), 0, 1 << 20) % (slack + 1)
    tallies = tallies.at[source_of].add(-shifted).at[sink].add(shifted)
    members = jnp.searchsorted(jnp.cumsum(tallies), jnp.arange(rows * top), side="right").astype(jnp.int32)
    table = members.reshape(top, rows).T
    table = table[jax.random.permutation(jax.random.fold_in(own, 1), rows)]
    turn = jax.random.randint(jax.random.fold_in(own, 2), (rows, 1), 0, top)
    return jnp.take_along_axis(table, (jnp.arange(top)[None, :] + turn) % top, axis=1)


def shares(number_of, total, limit, skew, full):
    weights = [(1 << 20) // math.isqrt(rank ** skew) + 1 for rank in range(1, number_of + 1)]
    largest = limit if full else min(limit, max(-(-total // number_of), total * weights[0] // sum(weights)))
    least = 1 if total - largest >= number_of - 1 else 0
    given, spare = [largest] + [least] * (number_of - 1), total - largest - least * (number_of - 1)
    while spare > 0:
        candidates = [i for i in range(1, number_of) if given[i] < largest] or [i for i in range(1, number_of) if given[i] < limit]
        mass, remaining = sum([weights[i] for i in candidates]), spare
        for i in candidates:
            more = min(limit - given[i], max(1, remaining * weights[i] // mass), spare)
            given[i] = given[i] + more
            spare = spare - more
    return np.array(given)


def noise(key, shape, scale, limit, cuts=(), kind=jnp.bfloat16):
    entries = scale * jax.random.normal(key, shape, jnp.float32)
    if cuts:
        entries = entries * block_scale(key, shape, cuts, -0.22, 0.18)
    return jnp.clip(entries, -limit, limit).astype(kind)


def setup_inputs(seed: int = 0) -> dict:
    arg_keys = jax.random.split(jax.random.key(seed), 7)
    tokens = noise(arg_keys[0], (TOKENS, D), 1.0, 6.0, ((0, 16), (1, 2)))
    expert_ids_keys = jax.random.split(jax.random.fold_in(arg_keys[1], 1), TOKENS // TOK_DEV)
    expert_ids_turns = jax.random.permutation(jax.random.fold_in(arg_keys[1], 3), TOKENS // TOK_DEV)
    expert_ids = jax.vmap(lambda own, number: routed_block(jax.random.fold_in(arg_keys[1], 2), own, number, TOK_DEV, EXPERTS, TOP, CAP, 2))(expert_ids_keys, expert_ids_turns).reshape((TOKENS, TOP))
    combine = jnp.clip(jnp.exp(math.log(1.0) - 2.9957323 * jax.random.uniform(arg_keys[2], (TOKENS, TOP), jnp.float32) ** block_scale(arg_keys[2], (TOKENS, TOP), ((0, 16),), -0.2, 0.2)), 0.05, 1.0)
    gate_weight = noise(arg_keys[3], (EXPERTS, D, FF), D ** -0.5, 0.09375, ((0, 8), (1, 2), (2, 2)))
    up_weight = noise(arg_keys[4], (EXPERTS, D, FF), D ** -0.5, 0.09375, ((0, 8), (1, 2), (2, 2)))
    down_weight = noise(arg_keys[5], (EXPERTS, FF, D), FF ** -0.5, 0.15625, ((0, 8), (1, 2), (2, 2)))
    return dict(tokens=tokens, expert_ids=expert_ids, combine=combine, gate_weight=gate_weight, up_weight=up_weight, down_weight=down_weight)


def reference(tokens, expert_ids, combine, gate_weight, up_weight, down_weight):
    tok_rows = tokens.shape[0]
    rows_max = N_DP * N_EXPERT * CAP
    share = FF // N_ETP

    def one_expert(running, expert):
        selected = expert_ids == expert
        chosen = jnp.any(selected, axis=1)
        weight = jnp.sum(jnp.where(selected, combine, 0.0), axis=1)
        ordering = jnp.cumsum(chosen.astype(jnp.int32)) - 1
        placement = jnp.where(chosen, ordering, rows_max).astype(jnp.int32)
        row_index = jnp.zeros((rows_max + 1,), jnp.int32).at[placement].set(jnp.arange(tok_rows, dtype=jnp.int32))
        row_block = tokens[row_index[:rows_max]]
        gate_sum = jnp.dot(row_block, gate_weight[expert], preferred_element_type=jnp.float32)
        up_sum = jnp.dot(row_block, up_weight[expert], preferred_element_type=jnp.float32)
        hidden = (jax.nn.silu(gate_sum) * up_sum).astype(jnp.bfloat16)
        summed = jnp.zeros((rows_max, tokens.shape[1]), jnp.float32)
        for shard in range(N_ETP):
            partial_value = jnp.dot(hidden[:, shard * share:(shard + 1) * share], down_weight[expert][shard * share:(shard + 1) * share], preferred_element_type=jnp.float32).astype(jnp.bfloat16)
            partial_value = lax.optimization_barrier(partial_value)
            summed = summed + partial_value.astype(jnp.float32)
        expert_out = summed.astype(jnp.bfloat16)
        gathered = expert_out[jnp.clip(ordering, 0, rows_max - 1)].astype(jnp.float32)
        running = running + jnp.where(chosen[:, None], weight[:, None] * gathered, 0.0)
        return running, None

    start_sum = jnp.zeros(tokens.shape, jnp.float32)
    total, unused = lax.scan(one_expert, start_sum, jnp.arange(gate_weight.shape[0], dtype=jnp.int32))
    return total.astype(jnp.bfloat16)
```

```python
import jax
import jax.numpy as jnp
from jax import lax
from jax.sharding import PartitionSpec as P


def spread_tokens(tokens, groups, cores, width):
    rows = tokens.shape[0]
    if groups == cores:
        perm = [
            (((d - c) % groups) * cores + d, d * cores + c)
            for d in range(groups)
            for c in range(cores)
        ]
        swapped = lax.ppermute(tokens, ("dp", "etp"), perm)
        along = lax.all_gather(swapped, "expert", axis=0)
        return lax.all_gather(along, "etp", axis=0)
    full = lax.all_gather(tokens, "etp", axis=1, tiled=True)
    mine = lax.all_to_all(
        full.reshape(rows, groups, width), "dp", split_axis=1, concat_axis=0, tiled=False
    )
    mine = mine.reshape(groups, rows, width)
    order = jnp.mod(lax.axis_index("dp") - jnp.arange(groups), groups)
    return lax.all_gather(jnp.take(mine, order, axis=0), "expert", axis=1)


def collect_output(parts, groups, cores, width):
    stacked = jnp.stack(parts)
    if groups == cores:
        summed = lax.psum_scatter(stacked, "etp", scatter_dimension=0, tiled=False)
        summed = lax.psum_scatter(summed, "expert", scatter_dimension=0, tiled=False)
        perm = [
            (d * cores + c, ((d - c) % groups) * cores + d)
            for d in range(groups)
            for c in range(cores)
        ]
        return lax.ppermute(summed, ("dp", "etp"), perm)
    summed = lax.psum_scatter(stacked, "expert", scatter_dimension=1, tiled=False)
    order = jnp.mod(lax.axis_index("dp") - jnp.arange(groups), groups)
    summed = lax.psum(jnp.take(summed, order, axis=0).astype(jnp.float32), "etp")
    back = lax.all_to_all(
        summed.astype(jnp.bfloat16), "dp", split_axis=0, concat_axis=1, tiled=True
    )
    back = back.reshape(back.shape[1] // groups, -1) if back.ndim == 2 else back
    rows = back.shape[-2] // groups
    back = back.reshape(groups, rows, width).transpose(1, 0, 2).reshape(rows, cores, -1)
    return lax.dynamic_index_in_dim(back, lax.axis_index("etp"), 1, keepdims=False)


def shards(tokens, expert_ids, combine, gate_weight, up_weight, down_weight):
    rows, top_count = expert_ids.shape
    held, width, _ = gate_weight.shape
    groups = lax.axis_size("dp")
    columns = lax.axis_size("expert")
    cores = lax.axis_size("etp")
    experts = held * columns
    capacity = min(rows, 3 * rows * top_count // (2 * experts))
    group = lax.axis_index("dp")

    named = expert_ids[:, :, None] == jnp.arange(experts, dtype=jnp.int32)[None, None, :]
    weight = jnp.sum(jnp.where(named, combine[:, :, None], 0.0), axis=1)
    weight = lax.all_gather(weight.T, ("dp", "expert"), axis=0)
    weight = lax.dynamic_slice_in_dim(weight, lax.axis_index("expert") * held, held, axis=1)
    chosen = (weight > 0).astype(jnp.bfloat16)
    earlier = jnp.triu(jnp.ones((rows, rows), jnp.bfloat16), 1)
    place = jnp.einsum("bet,tu->beu", chosen, earlier, preferred_element_type=jnp.float32)
    slots = jnp.arange(capacity, dtype=jnp.float32)[None, None, :, None]
    hit = (place[:, :, None, :] == slots) & (weight > 0)[:, :, None, :]
    picker = hit.astype(jnp.bfloat16).reshape(groups, columns, held, capacity, rows)
    slot_weight = jnp.sum(jnp.where(hit, weight[:, :, None, :], 0.0), axis=-1)
    slot_weight = slot_weight.reshape(groups, columns, held, capacity)

    spread = spread_tokens(tokens, groups, cores, width)

    def pick(r):
        which = jnp.mod(group - r, groups)
        return lax.dynamic_index_in_dim(picker, which, 0, keepdims=False)

    def gate_up(r):
        packed = jnp.einsum(
            "xest,xtk->exsk", pick(r), spread[r], preferred_element_type=jnp.float32
        )
        packed = packed.astype(jnp.bfloat16).reshape(held, columns * capacity, width)
        found = []
        for e in range(held):
            found.append(
                tuple(
                    jnp.dot(packed[e], w[e], preferred_element_type=jnp.float32)
                    for w in (gate_weight, up_weight)
                )
            )
        return found

    gates = [[] for _ in range(held)]
    ups = [[] for _ in range(held)]
    for r in range(1, groups):
        perm = [(d, (d - r) % groups) for d in range(groups)]
        for e, (g, u) in enumerate(gate_up(r)):
            sent = lax.ppermute(
                jnp.concatenate([g, u], axis=1).astype(jnp.bfloat16), "dp", perm
            )
            half = sent.shape[1] // 2
            gates[e].append(sent[:, :half].astype(jnp.float32))
            ups[e].append(sent[:, half:].astype(jnp.float32))
    own_weight = lax.dynamic_index_in_dim(slot_weight, group, 0, keepdims=False)
    own_weight = own_weight.transpose(1, 0, 2).reshape(held, columns * capacity, 1)
    hidden = [[] for _ in range(groups)]
    for e, (g, u) in enumerate(gate_up(0)):
        g = sum(gates[e], g)
        u = sum(ups[e], u)
        h = (jax.nn.silu(g) * u * own_weight[e]).astype(jnp.bfloat16)
        hidden[0].append(h)
        for r in range(1, groups):
            perm = [(d, (d + r) % groups) for d in range(groups)]
            hidden[r].append(lax.ppermute(h, "dp", perm))

    parts = []
    for r in range(groups):
        h = jnp.stack(hidden[r]).reshape(held, columns, capacity, -1)
        dense = jnp.einsum("xest,exsf->xtef", pick(r), h, preferred_element_type=jnp.float32)
        dense = dense.astype(jnp.bfloat16).reshape(columns * rows, -1)
        out = jnp.dot(
            dense, down_weight.reshape(-1, width), preferred_element_type=jnp.float32
        )
        parts.append(out.astype(jnp.bfloat16).reshape(columns, rows, width))
    return collect_output(parts, groups, cores, width)


def solution(mesh):
    placed = (
        P(("dp", "expert"), "etp"),
        P(("dp", "expert"), None),
        P(("dp", "expert"), None),
        P("expert", "dp", "etp"),
        P("expert", "dp", "etp"),
        P("expert", "etp", "dp"),
    )
    return jax.shard_map(
        shards, mesh=mesh, in_specs=placed, out_specs=P(("dp", "expert"), "etp"), check_vma=False
    )
```

```python
import jax
import jax.numpy as jnp
from jax import lax
from jax.sharding import PartitionSpec as P


def ring_steps(columns):
    ring = list(range(0, columns, 2)) + list(range(1, columns, 2))[::-1]
    ahead = [(ring[i], ring[(i + 1) % columns]) for i in range(columns)]
    return ahead, [(b, a) for a, b in ahead]


def ring_spread(block, groups, columns, cores):
    perm = [
        (((d - c) % groups) * cores + d, d * cores + c) for d in range(groups) for c in range(cores)
    ]
    ahead, back = ring_steps(columns)
    block = lax.ppermute(block, ("dp", "etp"), perm)
    held = {0: block}
    up = down = block
    for step in range(1, columns // 2 + 1):
        up = lax.ppermute(up, "expert", ahead)
        held[step] = up
        if columns - step > step:
            down = lax.ppermute(down, "expert", back)
            held[columns - step] = down
    swap = [(0, 1), (1, 0)]
    other = {k: lax.ppermute(held[k], "etp", swap) for k in held}
    first = lax.axis_index("etp") == 0
    pairs = [(held[k], other[k]) for k in range(columns)]
    return (
        jnp.stack([jnp.where(first, a, b) for a, b in pairs]),
        jnp.stack([jnp.where(first, b, a) for a, b in pairs]),
    )


def ring_collect(parts, groups, columns, cores):
    ahead, back = ring_steps(columns)
    first = lax.axis_index("etp") == 0
    mine = jnp.where(first, parts[0], parts[1])
    away = jnp.where(first, parts[1], parts[0])
    half = mine.shape[1] // 2
    order = [k for s in range(1, columns // 2 + 1) for k in (s, columns - s)] + [0]
    other = {}
    for k in order:
        if k not in other:
            other[k] = lax.ppermute(away[k], "etp", [(0, 1), (1, 0)])

    def own(k, low):
        rows = slice(0, half) if low else slice(half, None)
        return mine[k, rows].astype(jnp.float32) + other[k][rows].astype(jnp.float32)

    up = own(1, True).astype(jnp.bfloat16)
    down = own(columns - 1, False).astype(jnp.bfloat16)
    for step in range(2, columns + 1):
        up = lax.ppermute(up, "expert", ahead)
        down = lax.ppermute(down, "expert", back)
        up = (up.astype(jnp.float32) + own(step % columns, True)).astype(jnp.bfloat16)
        down = (down.astype(jnp.float32) + own(columns - step, False)).astype(jnp.bfloat16)
    perm = [
        (d * cores + c, ((d - c) % groups) * cores + d) for d in range(groups) for c in range(cores)
    ]
    return lax.ppermute(jnp.concatenate([up, down]), ("dp", "etp"), perm)


def spread_tokens(tokens, groups, cores, width):
    rows = tokens.shape[0]
    if groups == cores:
        perm = [
            (((d - c) % groups) * cores + d, d * cores + c)
            for d in range(groups)
            for c in range(cores)
        ]
        swapped = lax.ppermute(tokens, ("dp", "etp"), perm)
        along = lax.all_gather(swapped, "expert", axis=0)
        return lax.all_gather(along, "etp", axis=0)
    full = lax.all_gather(tokens, "etp", axis=1, tiled=True)
    mine = lax.all_to_all(
        full.reshape(rows, groups, width), "dp", split_axis=1, concat_axis=0, tiled=False
    )
    mine = mine.reshape(groups, rows, width)
    order = jnp.mod(lax.axis_index("dp") - jnp.arange(groups), groups)
    return lax.all_gather(jnp.take(mine, order, axis=0), "expert", axis=1)


def collect_output(parts, groups, cores, width):
    stacked = jnp.stack(parts)
    if groups == cores:
        summed = lax.psum_scatter(stacked, "etp", scatter_dimension=0, tiled=False)
        summed = lax.psum_scatter(summed, "expert", scatter_dimension=0, tiled=False)
        perm = [
            (d * cores + c, ((d - c) % groups) * cores + d)
            for d in range(groups)
            for c in range(cores)
        ]
        return lax.ppermute(summed, ("dp", "etp"), perm)
    summed = lax.psum_scatter(stacked, "expert", scatter_dimension=1, tiled=False)
    order = jnp.mod(lax.axis_index("dp") - jnp.arange(groups), groups)
    summed = lax.psum(jnp.take(summed, order, axis=0).astype(jnp.float32), "etp")
    back = lax.all_to_all(
        summed.astype(jnp.bfloat16), "dp", split_axis=0, concat_axis=1, tiled=True
    )
    back = back.reshape(back.shape[1] // groups, -1) if back.ndim == 2 else back
    rows = back.shape[-2] // groups
    back = back.reshape(groups, rows, width).transpose(1, 0, 2).reshape(rows, cores, -1)
    return lax.dynamic_index_in_dim(back, lax.axis_index("etp"), 1, keepdims=False)


def shards(tokens, expert_ids, combine, gate_weight, up_weight, down_weight):
    rows, top_count = expert_ids.shape
    held, width, _ = gate_weight.shape
    groups = lax.axis_size("dp")
    columns = lax.axis_size("expert")
    cores = lax.axis_size("etp")
    experts = held * columns
    capacity = min(rows, 3 * rows * top_count // (2 * experts))
    group = lax.axis_index("dp")

    named = expert_ids[:, :, None] == jnp.arange(experts, dtype=jnp.int32)[None, None, :]
    weight = jnp.sum(jnp.where(named, combine[:, :, None], 0.0), axis=1)
    near = groups == cores == 2 and columns % 2 == 0
    if near:
        high = weight.T.astype(jnp.bfloat16)
        low = (weight.T - high.astype(jnp.float32)).astype(jnp.bfloat16)
        extra = jnp.stack([high, low]).reshape(-1)
        extra_rows = -(-extra.size // (8 * tokens.shape[1])) * 8
        extra = jnp.pad(extra, (0, extra_rows * tokens.shape[1] - extra.size))
        block = jnp.concatenate([tokens, extra.reshape(extra_rows, -1)])
        whole = ring_spread(block, groups, columns, cores)
        spread = [a[:, :rows] for a in whole]
        tail = jnp.stack([a[:, rows:] for a in whole]).reshape(groups * columns, -1)
        tail = tail[:, : 2 * experts * rows].reshape(-1, 2, experts, rows).astype(jnp.float32)
        weight = tail[:, 0] + tail[:, 1]
    else:
        spread = spread_tokens(tokens, groups, cores, width)
        weight = lax.all_gather(weight.T, ("dp", "expert"), axis=0)
    weight = lax.dynamic_slice_in_dim(weight, lax.axis_index("expert") * held, held, axis=1)
    chosen = (weight > 0).astype(jnp.bfloat16)
    earlier = jnp.triu(jnp.ones((rows, rows), jnp.bfloat16), 1)
    place = jnp.einsum("bet,tu->beu", chosen, earlier, preferred_element_type=jnp.float32)
    slots = jnp.arange(capacity, dtype=jnp.float32)[None, None, :, None]
    hit = (place[:, :, None, :] == slots) & (weight > 0)[:, :, None, :]
    picker = hit.astype(jnp.bfloat16).reshape(groups, columns, held, capacity, rows)
    slot_weight = jnp.sum(jnp.where(hit, weight[:, :, None, :], 0.0), axis=-1)
    slot_weight = slot_weight.reshape(groups, columns, held, capacity)

    def pick(r):
        which = r if near else jnp.mod(group - r, groups)
        return lax.dynamic_index_in_dim(picker, which, 0, keepdims=False)

    def gate_up(r):
        packed = jnp.einsum(
            "xest,xtk->exsk", pick(r), spread[r], preferred_element_type=jnp.float32
        )
        packed = packed.astype(jnp.bfloat16).reshape(held, columns * capacity, width)
        found = []
        for e in range(held):
            found.append(
                tuple(
                    jnp.dot(packed[e], w[e], preferred_element_type=jnp.float32)
                    for w in (gate_weight, up_weight)
                )
            )
        return found

    gates = [[] for _ in range(held)]
    ups = [[] for _ in range(held)]
    for r in range(1, groups):
        perm = [(d, (d - r) % groups) for d in range(groups)]
        for e, (g, u) in enumerate(gate_up(r)):
            sent = lax.ppermute(
                jnp.concatenate([g, u], axis=1).astype(jnp.bfloat16), "dp", perm
            )
            half = sent.shape[1] // 2
            gates[e].append(sent[:, :half].astype(jnp.float32))
            ups[e].append(sent[:, half:].astype(jnp.float32))
    own_weight = lax.dynamic_index_in_dim(slot_weight, 0 if near else group, 0, keepdims=False)
    own_weight = own_weight.transpose(1, 0, 2).reshape(held, columns * capacity, 1)
    hidden = [[] for _ in range(groups)]
    for e, (g, u) in enumerate(gate_up(0)):
        g = sum(gates[e], g)
        u = sum(ups[e], u)
        h = (jax.nn.silu(g) * u * own_weight[e]).astype(jnp.bfloat16)
        hidden[0].append(h)
        for r in range(1, groups):
            perm = [(d, (d + r) % groups) for d in range(groups)]
            hidden[r].append(lax.ppermute(h, "dp", perm))

    parts = []
    for r in range(groups):
        h = jnp.stack(hidden[r]).reshape(held, columns, capacity, -1)
        dense = jnp.einsum("xest,exsf->xtef", pick(r), h, preferred_element_type=jnp.float32)
        dense = dense.astype(jnp.bfloat16).reshape(columns * rows, -1)
        out = jnp.dot(
            dense, down_weight.reshape(-1, width), preferred_element_type=jnp.float32
        )
        parts.append(out.astype(jnp.bfloat16).reshape(columns, rows, width))
    if near:
        return ring_collect(parts, groups, columns, cores)
    return collect_output(parts, groups, cores, width)


def solution(mesh):
    placed = (
        P(("dp", "expert"), "etp"),
        P(("dp", "expert"), None),
        P(("dp", "expert"), None),
        P("expert", "dp", "etp"),
        P("expert", "dp", "etp"),
        P("expert", "etp", "dp"),
    )
    return jax.shard_map(
        shards, mesh=mesh, in_specs=placed, out_specs=P(("dp", "expert"), "etp"), check_vma=False
    )
```
